128 devices in a mesh: asset: 32 (over y, z, core), tm: 4 (over x).
Axes of the slice: x: 4, y: 4, z: 4, core: 2. Of those that a mesh axis runs over, the one named last changes fastest.
Arguments:
- values: float32 [4, 1024, 65536], P(None, 'tm', 'asset'), may hold values from -64 to 64
- listed_from: int32 [65536], P('asset'), may hold values from -1024 to 1023, as said below
- listed_until: int32 [65536], P('asset'), may hold values from -960 to 3070, as said below
Outputs:
- standardized: float32 [4, 1024, 65536], P(None, 'tm', 'asset')
The draws below stay inside these ranges and needn't reach their ends.
Inputs may be any that keep to these rules, and one draw needn't show every extreme that they name: listed_until[a] - listed_from[a] is at least 64. listed_until[a] - listed_from[a] is at least 64.
All inputs are finite; a program needn't handle non-finite values.
Results may differ from the reference program's by a relative error of at most 0.00005.
Values sent between devices are 32-bit elements; how exact they have to be, the bound alone decides.
A program may use at most 128 MiB of HBM per device.

```python
import jax
import jax.numpy as jnp
from jax import lax

F = 4
WINDOW = 64
TIME = 1024
ASSETS = 65536


def listing_dates(key):
    base = jax.random.fold_in(key, 7)
    key_start, key_length = jax.random.split(base)
    first_stamp = jax.random.randint(key_start, (ASSETS,), -TIME, TIME, dtype=jnp.int32)
    length = jax.random.randint(key_length, (ASSETS,), WINDOW, 2 * TIME, dtype=jnp.int32)
    return (first_stamp, first_stamp + length)


def draw_listed_from(key, part):
    return listing_dates(key)[0]


def draw_listed_until(key, part):
    return listing_dates(key)[1]


def draw_values(key, part):
    base = jax.random.fold_in(key, 11)
    key_noise, key_scale, key_common, key_drift = jax.random.split(base, 4)
    noise_draw = jax.random.normal(key_noise, (F, TIME, ASSETS), jnp.float32)
    field_values = 8.0 * noise_draw
    return jnp.clip(field_values, -64.0, 64.0)


def setup_inputs(seed: int = 0) -> dict:
    arg_keys = jax.random.split(jax.random.key(seed), 4)
    values = draw_values(jax.random.fold_in(arg_keys[3], 71), 0)
    listed_from = draw_listed_from(jax.random.fold_in(arg_keys[3], 71), 0)
    listed_until = draw_listed_until(jax.random.fold_in(arg_keys[3], 71), 0)
    return {"values": values, "listed_from": listed_from, "listed_until": listed_until}


def standardize(field_values, weight, present):
    center = lax.optimization_barrier(jnp.sum(weight * field_values, axis=1)) / present
    deviate = (field_values - center[:, None]) * weight
    spread = lax.optimization_barrier(jnp.sum(deviate * deviate, axis=1)) / present
    return deviate / jnp.sqrt(spread + 0.1)[:, None]

def reference(values, listed_from, listed_until):
    stamps = jnp.arange(TIME, dtype=jnp.int32)[:, None]
    opened = listed_from[None, :]
    closed = listed_until[None, :]
    weight = ((stamps >= opened) & (stamps < closed)).astype(values.dtype)
    window_low = jnp.maximum(jnp.maximum(stamps - (WINDOW - 1), opened), 0)
    window_high = jnp.minimum(stamps, closed - 1)
    counted = jnp.maximum(window_high - window_low + 1, 1).astype(values.dtype)
    present = jnp.maximum(lax.optimization_barrier(jnp.sum(weight, axis=1)), 1.0)

    def one_field(field_values):
        window_sum = lax.reduce_window(field_values * weight, jnp.zeros((), field_values.dtype), lax.add, (WINDOW, 1), (1, 1), ((WINDOW - 1, 0), (0, 0)))
        rolling = window_sum / counted
        clipped = jnp.clip(standardize(rolling, weight, present), -3.0, 3.0)
        return standardize(clipped, weight, present)
    return lax.map(one_field, values)
```

```python
import functools

import jax
import jax.numpy as jnp
from jax import lax
from jax.experimental import pallas as pl
from jax.experimental.pallas import tpu as pltpu
from jax.sharding import PartitionSpec as P

WINDOW = 64
LANES = 128
CLIP = 3.0
UNROLL = 4
LINE = 8


def field_groups(fields):
    half = (fields + 1) // 2
    return [(start, min(half, fields - start)) for start in range(0, fields, half)]


def kernel(
    n_tm, n_as, values, opened_hbm, closed_hbm, out,
    x, rolling, weight, inverse, opened_ref, closed_ref, stage,
    part, got, totals, tail_part, tail_got, tail_totals,
    load_sem, halo_send, halo_recv, next_sem, done_sem, ready,
    send_sem, recv_sem, tail_send, tail_recv,
):
    fields, rows, assets = values.shape
    blocks = rows // WINDOW
    chunks = assets // LANES
    groups = field_groups(fields)
    ahead = fields - 1
    tm = lax.axis_index("tm")
    me = lax.axis_index("asset")
    later = lax.rem(tm + 1, n_tm)
    before = lax.rem(tm + n_tm - 1, n_tm)
    is_first = tm == 0
    is_last = tm == n_tm - 1
    spot = lax.rem(me, LINE)
    line_peers = [me - spot + lax.rem(spot + d, LINE) for d in range(1, LINE)]
    cross_peers = [lax.rem(me + LINE * d, n_as) for d in range(1, n_as // LINE)]

    dates = [
        pltpu.make_async_copy(opened_hbm, opened_ref, load_sem.at[fields]),
        pltpu.make_async_copy(closed_hbm, closed_ref, load_sem.at[fields + 1]),
    ]
    loads = [
        pltpu.make_async_copy(values.at[f], x.at[f, pl.ds(WINDOW, rows)], load_sem.at[f])
        for f in range(fields)
    ]

    barrier = pltpu.get_barrier_semaphore()
    for other in (later, before):
        pl.semaphore_signal(barrier, inc=1, device_id={"tm": other})
    for other in line_peers + cross_peers:
        pl.semaphore_signal(barrier, inc=1, device_id={"asset": other})
    for copy in dates + loads:
        copy.start()
    pl.semaphore_wait(barrier, 2 + len(line_peers) + len(cross_peers))

    halos = [
        pltpu.make_async_remote_copy(
            src_ref=values.at[f, pl.ds(rows - WINDOW, WINDOW)],
            dst_ref=x.at[f, pl.ds(0, WINDOW)],
            send_sem=halo_send.at[f],
            recv_sem=halo_recv.at[f],
            device_id={"tm": later},
        )
        for f in range(fields - 1)
    ]
    upcoming = pltpu.make_async_remote_copy(
        src_ref=values.at[ahead, pl.ds(0, WINDOW)],
        dst_ref=x.at[ahead, pl.ds(WINDOW + rows, WINDOW)],
        send_sem=next_sem.at[0],
        recv_sem=next_sem.at[1],
        device_id={"tm": before},
    )
    finished = pltpu.make_async_remote_copy(
        src_ref=stage,
        dst_ref=out.at[ahead, pl.ds(0, WINDOW)],
        send_sem=done_sem.at[0],
        recv_sem=done_sem.at[1],
        device_id={"tm": later},
    )
    pl.when(jnp.logical_not(is_first))(upcoming.start)
    for copy in halos:
        copy.start()
    for other in cross_peers:
        pl.semaphore_signal(ready, inc=1, device_id={"asset": other})

    def send(slot):
        for d in range(1, n_as):
            pltpu.make_async_remote_copy(
                src_ref=part.at[slot],
                dst_ref=got.at[slot, d - 1],
                send_sem=send_sem.at[slot],
                recv_sem=recv_sem.at[slot],
                device_id={"asset": lax.rem(me + d, n_as)},
            ).start()

    def receive(slot):
        arrived = got.at[slot]
        pltpu.make_async_copy(arrived, arrived, recv_sem.at[slot]).wait()
        return part[slot] + jnp.sum(got[slot], axis=0)

    def send_row(slot):
        for d in range(1, n_as):
            pltpu.make_async_remote_copy(
                src_ref=tail_part.at[slot],
                dst_ref=tail_got.at[slot, pl.ds(d - 1, 1)],
                send_sem=tail_send.at[slot],
                recv_sem=tail_recv.at[slot],
                device_id={"asset": lax.rem(me + d, n_as)},
            ).start()

    def receive_row(slot):
        arrived = tail_got.at[slot]
        pltpu.make_async_copy(arrived, arrived, tail_recv.at[slot]).wait()
        tail_totals[slot] = tail_part[slot] + jnp.sum(tail_got[slot], axis=0, keepdims=True)

    def row_of(first, second):
        return jnp.sum(jnp.concatenate([first, second], axis=0).T, axis=0, keepdims=True)

    def factors(row, count):
        mean = row / jnp.maximum(count, 1.0)
        other = pltpu.roll(mean, WINDOW, 1)
        scale = 1.0 / jnp.sqrt(jnp.maximum(mean - other * other, 0.0) + 0.1)
        lane = lax.broadcasted_iota(jnp.int32, row.shape, 1)
        both = jnp.broadcast_to(jnp.where(lane < WINDOW, mean, scale), (LANES, LANES)).T
        return both[:WINDOW], both[WINDOW:]

    def columns(c):
        return pl.ds(pl.multiple_of(c * LANES, LANES), LANES)

    zero = jnp.zeros((WINDOW, LANES), jnp.float32)
    part[...] = jnp.zeros(part.shape, part.dtype)

    @pl.when(is_first)
    def no_past():
        x[ahead, :WINDOW, :] = jnp.zeros((WINDOW, assets), jnp.float32)

    first_stamp = tm * rows - WINDOW
    for copy in dates:
        copy.wait()

    @pl.loop(0, blocks + 2)
    def listing(b):
        start = pl.multiple_of(b * WINDOW, WINDOW)
        stamps = first_stamp + start + lax.broadcasted_iota(jnp.int32, (WINDOW, LANES), 0)

        def chunk(c, total):
            cols = columns(c)
            opened = jnp.maximum(opened_ref[:, cols], 0)
            closed = closed_ref[:, cols]
            listed = (stamps >= opened) & (stamps < closed)
            low = jnp.maximum(stamps - (WINDOW - 1), opened)
            counted = jnp.maximum(jnp.minimum(stamps + 1, closed) - low, 1).astype(jnp.float32)
            ones = jnp.where(listed, 1.0, 0.0)
            weight[pl.ds(start, WINDOW), cols] = ones
            inverse[pl.ds(start, WINDOW), cols] = ones / counted
            return total + ones

        total = lax.fori_loop(0, chunks, chunk, zero, unroll=2)
        part[0, pl.ds(lax.rem(b + blocks + 1, blocks + 2), 1), :] = row_of(total, total)

    pl.semaphore_wait(ready, len(cross_peers))
    send(0)

    def roll_window(f, b):
        top = pl.multiple_of(b * WINDOW, WINDOW)

        def chunk(c, carry):
            cols = columns(c)
            reach = pl.ds(top, 2 * WINDOW)
            sums = x[f, reach, cols] * weight[reach, cols]
            for step in (8, 16, 32):
                sums = sums[step:] + sums[:-step]
            for step in (1, 2, 4):
                sums = sums + pltpu.roll(sums, step, 0)
            means = sums[8:] * inverse[pl.ds(top + WINDOW, WINDOW), cols]
            rolling[f, pl.ds(top, WINDOW), cols] = means
            return carry[0] + means, carry[1] + means * means

        return row_of(*lax.fori_loop(0, chunks, chunk, (zero, zero), unroll=UNROLL))

    def clip_scores(f, b, center, scale):
        top = pl.multiple_of(b * WINDOW, WINDOW)

        def chunk(c, carry):
            cols = columns(c)
            scored = (rolling[f, pl.ds(top, WINDOW), cols] - center) * scale
            clipped = jnp.minimum(jnp.maximum(scored, -CLIP), CLIP)
            masked = clipped * weight[pl.ds(top + WINDOW, WINDOW), cols]
            return carry[0] + masked, carry[1] + masked * clipped

        return row_of(*lax.fori_loop(0, chunks, chunk, (zero, zero), unroll=UNROLL))

    def finish(f, b, first, second, target, base):
        top = pl.multiple_of(b * WINDOW, WINDOW)
        base = pl.multiple_of(base, WINDOW)
        center, scale = first
        middle, factor = second

        @pl.loop(0, chunks, unroll=UNROLL)
        def chunk(c):
            cols = columns(c)
            scored = (rolling[f, pl.ds(top, WINDOW), cols] - center) * scale
            clipped = jnp.minimum(jnp.maximum(scored, -CLIP), CLIP)
            deviate = (clipped - middle) * weight[pl.ds(top + WINDOW, WINDOW), cols]
            target[pl.ds(base, WINDOW), cols] = deviate * factor

    def count_row(b):
        return totals[0, pl.ds(b, 1), :]

    def total_row(slot, i):
        return totals[slot, pl.ds(i, 1), :]

    def items(g):
        start, size = groups[g]
        whole = size * (blocks - 1)
        if start + size < fields:
            return whole, lambda i: (start + lax.rem(i, size), 1 + lax.div(i, size))
        return whole + is_first.astype(jnp.int32), lambda i: (
            jnp.where(i < whole, start + lax.rem(i, size), ahead),
            jnp.where(i < whole, 1 + lax.div(i, size), 0),
        )

    def main_first(g):
        start, size = groups[g]
        for f in range(start, start + size):
            loads[f].wait()
        number, place = items(g)

        @pl.loop(0, number)
        def item(i):
            f, b = place(i)
            part[1 + 2 * g, pl.ds(i, 1), :] = roll_window(f, b)

        send(1 + 2 * g)

    def main_second(g):
        slot = 1 + 2 * g
        totals[slot] = receive(slot)
        number, place = items(g)

        @pl.loop(0, number)
        def item(i):
            f, b = place(i)
            center, scale = factors(total_row(slot, i), count_row(b))
            part[slot + 1, pl.ds(i, 1), :] = clip_scores(f, b, center, scale)

        send(slot + 1)

    def main_third(g):
        slot = 1 + 2 * g
        totals[slot + 1] = receive(slot + 1)
        number, place = items(g)

        @pl.loop(0, number)
        def item(i):
            f, b = place(i)
            count = count_row(b)
            first = factors(total_row(slot, i), count)
            second = factors(total_row(slot + 1, i), count)
            finish(f, b, first, second, out.at[f], b * WINDOW)

    def tail_first(f, b):
        tail_part[2 * f] = roll_window(f, b)
        send_row(2 * f)

    def tail_second(f, b):
        slot = 2 * f
        receive_row(slot)
        center, scale = factors(tail_totals[slot], count_row(b))
        tail_part[slot + 1] = clip_scores(f, b, center, scale)
        send_row(slot + 1)

    def tail_third(f, b, target):
        slot = 2 * f
        receive_row(slot + 1)
        count = count_row(b)
        first = factors(tail_totals[slot], count)
        second = factors(tail_totals[slot + 1], count)
        finish(f, b, first, second, target, 0)

    def ahead_first():
        upcoming.wait_recv()
        tail_first(ahead, blocks)

    def ahead_second():
        tail_second(ahead, blocks)

    def ahead_third():
        tail_third(ahead, blocks, stage)
        finished.start()

    not_last = pl.when(jnp.logical_not(is_last))

    def first(f):
        halos[f].wait_recv()
        tail_first(f, 0)

    def second(f):
        tail_second(f, 0)

    def third(f):
        tail_third(f, 0, out.at[f])

    main_first(0)
    main_first(1)
    totals[0] = receive(0)
    main_second(0)
    not_last(ahead_first)
    main_second(1)
    first(0)
    not_last(ahead_second)
    main_third(0)
    second(0)
    not_last(ahead_third)
    main_third(1)
    third(0)
    for f in range(1, fields - 1):
        first(f)
        second(f)
        third(f)

    @pl.when(jnp.logical_not(is_first))
    def arrivals():
        finished.wait_recv()
        upcoming.wait_send()

    for copy in halos:
        copy.wait_send()
    for slot in range(part.shape[0]):
        sent = got.at[slot]
        pltpu.make_async_copy(sent, sent, send_sem.at[slot]).wait()

    def row_sent(slot):
        sent = tail_got.at[slot]
        pltpu.make_async_copy(sent, sent, tail_send.at[slot]).wait()

    for slot in range(2 * ahead):
        row_sent(slot)

    @not_last
    def departures():
        finished.wait_send()
        row_sent(2 * ahead)
        row_sent(2 * ahead + 1)


def per_device(n_tm, n_as, values, listed_from, listed_until):
    fields, rows, assets = values.shape
    blocks = rows // WINDOW
    groups = field_groups(fields)
    stats = -(-max(groups[0][1] * (blocks - 1) + 1, blocks + 2) // 8) * 8
    slots = 1 + 2 * len(groups)
    f32 = jnp.float32
    vmem = pltpu.VMEM
    dma = pltpu.SemaphoreType.DMA
    return pl.pallas_call(
        functools.partial(kernel, n_tm, n_as),
        out_shape=vmem((fields, rows, assets), f32),
        in_specs=[pl.BlockSpec(memory_space=pltpu.HBM)] * 3,
        out_specs=pl.BlockSpec(memory_space=vmem),
        scratch_shapes=[
            vmem((fields, rows + 2 * WINDOW, assets), f32),
            vmem((fields, rows + WINDOW, assets), f32),
            vmem((rows + 2 * WINDOW, assets), f32),
            vmem((rows + 2 * WINDOW, assets), f32),
            vmem((1, assets), jnp.int32),
            vmem((1, assets), jnp.int32),
            vmem((WINDOW, assets), f32),
            vmem((slots, stats, LANES), f32),
            vmem((slots, n_as - 1, stats, LANES), f32),
            vmem((slots, stats, LANES), f32),
            vmem((2 * fields, 1, LANES), f32),
            vmem((2 * fields, n_as - 1, LANES), f32),
            vmem((2 * fields, 1, LANES), f32),
            dma((fields + 2,)),
            dma((fields,)),
            dma((fields,)),
            dma((2,)),
            dma((2,)),
            pltpu.SemaphoreType.REGULAR,
            dma((slots,)),
            dma((slots,)),
            dma((2 * fields,)),
            dma((2 * fields,)),
        ],
        compiler_params=pltpu.CompilerParams(
            collective_id=0, has_side_effects=True, vmem_limit_bytes=48 * 2**20
        ),
    )(values, listed_from[None], listed_until[None])


def solution(mesh):
    in_specs = (P(None, "tm", "asset"), P("asset"), P("asset"))
    out_specs = P(None, "tm", "asset")
    body = functools.partial(per_device, mesh.shape["tm"], mesh.shape["asset"])
    return jax.shard_map(
        body, mesh=mesh, in_specs=in_specs, out_specs=out_specs, check_vma=False
    )
```

```python
import functools

import jax
import jax.numpy as jnp
from jax import lax
from jax.experimental import pallas as pl
from jax.experimental.pallas import tpu as pltpu
from jax.sharding import PartitionSpec as P

WINDOW = 64
LANES = 128
CLIP = 3.0
UNROLL = 4
LINE = 8
DIRECT = 1280


def field_groups(fields):
    half = (fields + 1) // 2
    return [(start, min(half, fields - start)) for start in range(0, fields, half)]


def kernel(
    n_tm, n_as, values, opened_hbm, closed_hbm, out,
    x, rolling, weight, inverse, opened_ref, closed_ref, stage, hold, lanes, spread,
    part, got, totals, tail_part, tail_got,
    load_sem, halo_send, halo_recv, next_sem, done_sem, hold_send, hold_recv, late_send, late_recv, ready,
    send_sem, recv_sem, tail_send, tail_recv,
):
    fields, rows, assets = values.shape
    blocks = rows // WINDOW
    chunks = assets // LANES
    groups = field_groups(fields)
    ahead = fields - 1
    tm = lax.axis_index("tm")
    me = lax.axis_index("asset")
    later = lax.rem(tm + 1, n_tm)
    before = lax.rem(tm + n_tm - 1, n_tm)
    across = lax.rem(tm + 2, n_tm)
    is_first = tm == 0
    is_last = tm == n_tm - 1
    spot = lax.rem(me, LINE)
    line_peers = [me - spot + lax.rem(spot + d, LINE) for d in range(1, LINE)]
    cross_peers = [lax.rem(me + LINE * d, n_as) for d in range(1, n_as // LINE)]

    dates = [
        pltpu.make_async_copy(opened_hbm, opened_ref, load_sem.at[fields]),
        pltpu.make_async_copy(closed_hbm, closed_ref, load_sem.at[fields + 1]),
    ]
    loads = [
        pltpu.make_async_copy(values.at[f], x.at[f, pl.ds(WINDOW, rows)], load_sem.at[f])
        for f in range(fields)
    ]

    barrier = pltpu.get_barrier_semaphore()
    for other in (later, before, across):
        pl.semaphore_signal(barrier, inc=1, device_id={"tm": other})
    for other in line_peers + cross_peers:
        pl.semaphore_signal(barrier, inc=1, device_id={"asset": other})
    for copy in dates + loads:
        copy.start()

    def columns(c):
        return pl.ds(pl.multiple_of(c * LANES, LANES), LANES)

    zero = jnp.zeros((WINDOW, LANES), jnp.float32)
    part[...] = jnp.zeros(part.shape, part.dtype)
    lanes[...] = jnp.zeros(lanes.shape, lanes.dtype)

    @pl.when(is_first)
    def no_past():
        x[ahead, :WINDOW, :] = jnp.zeros((WINDOW, assets), jnp.float32)
        x[ahead - 1, :WINDOW, DIRECT:] = jnp.zeros((WINDOW, assets - DIRECT), jnp.float32)

    first_stamp = tm * rows - WINDOW
    for copy in dates:
        copy.wait()

    @pl.loop(0, blocks + 2)
    def listing(b):
        start = pl.multiple_of(b * WINDOW, WINDOW)
        stamps = first_stamp + start + lax.broadcasted_iota(jnp.int32, (WINDOW, LANES), 0)

        def chunk(c, total):
            cols = columns(c)
            opened = jnp.maximum(opened_ref[:, cols], 0)
            closed = closed_ref[:, cols]
            listed = (stamps >= opened) & (stamps < closed)
            low = jnp.maximum(stamps - (WINDOW - 1), opened)
            counted = jnp.maximum(jnp.minimum(stamps + 1, closed) - low, 1).astype(jnp.float32)
            ones = jnp.where(listed, 1.0, 0.0)
            weight[pl.ds(start, WINDOW), cols] = ones
            inverse[pl.ds(start, WINDOW), cols] = ones / counted
            return total + ones

        total = lax.fori_loop(0, chunks, chunk, zero, unroll=2)
        here = lax.rem(b + blocks + 1, blocks + 2)
        lanes[0, here, :WINDOW] = total
        lanes[0, here, WINDOW:] = total

    pl.semaphore_wait(barrier, 3 + len(line_peers) + len(cross_peers))

    past = pl.ds(rows - WINDOW, WINDOW)
    direct = [pl.ds(0, assets if f < ahead - 1 else DIRECT) for f in range(ahead)]
    rest = pl.ds(DIRECT, assets - DIRECT)
    halos = [
        pltpu.make_async_remote_copy(
            src_ref=values.at[f, past, direct[f]],
            dst_ref=x.at[f, pl.ds(0, WINDOW), direct[f]],
            send_sem=halo_send.at[f],
            recv_sem=halo_recv.at[f],
            device_id={"tm": later},
        )
        for f in range(fields - 1)
    ]
    upcoming = pltpu.make_async_remote_copy(
        src_ref=values.at[ahead, pl.ds(0, WINDOW)],
        dst_ref=x.at[ahead, pl.ds(WINDOW + rows, WINDOW)],
        send_sem=next_sem.at[0],
        recv_sem=next_sem.at[1],
        device_id={"tm": before},
    )
    finished = pltpu.make_async_remote_copy(
        src_ref=stage,
        dst_ref=out.at[ahead, pl.ds(0, WINDOW)],
        send_sem=done_sem.at[0],
        recv_sem=done_sem.at[1],
        device_id={"tm": later},
    )

    def detour(slot, other):
        return pltpu.make_async_remote_copy(
            src_ref=values.at[ahead - 1, past, rest],
            dst_ref=hold.at[slot],
            send_sem=hold_send.at[0],
            recv_sem=hold_recv.at[slot],
            device_id={"tm": other},
        )

    def onward(slot, other):
        return pltpu.make_async_remote_copy(
            src_ref=hold.at[slot],
            dst_ref=x.at[ahead - 1, pl.ds(0, WINDOW), rest],
            send_sem=late_send.at[slot],
            recv_sem=late_recv.at[0],
            device_id={"tm": other},
        )

    is_even = lax.rem(tm, 2) == 0
    even_detour, odd_detour = detour(0, before), detour(1, across)
    cross_onward, back_onward = onward(0, across), onward(1, before)

    pl.when(jnp.logical_not(is_first))(upcoming.start)
    pl.when(is_even)(even_detour.start)
    pl.when(tm == 1)(odd_detour.start)
    for copy in halos:
        copy.start()
    for other in cross_peers:
        pl.semaphore_signal(ready, inc=1, device_id={"asset": other})

    def send(slot):
        for d in range(1, n_as):
            pltpu.make_async_remote_copy(
                src_ref=part.at[slot],
                dst_ref=got.at[slot, d - 1],
                send_sem=send_sem.at[slot],
                recv_sem=recv_sem.at[slot],
                device_id={"asset": lax.rem(me + d, n_as)},
            ).start()

    def receive(slot):
        arrived = got.at[slot]
        pltpu.make_async_copy(arrived, arrived, recv_sem.at[slot]).wait()
        return part[slot] + jnp.sum(got[slot], axis=0)

    def send_row(slot):
        for d in range(1, n_as):
            pltpu.make_async_remote_copy(
                src_ref=tail_part.at[slot],
                dst_ref=tail_got.at[slot, pl.ds(d - 1, 1)],
                send_sem=tail_send.at[slot],
                recv_sem=tail_recv.at[slot],
                device_id={"asset": lax.rem(me + d, n_as)},
            ).start()

    def receive_row(slot):
        arrived = tail_got.at[slot]
        pltpu.make_async_copy(arrived, arrived, tail_recv.at[slot]).wait()
        return tail_part[slot] + jnp.sum(tail_got[slot], axis=0, keepdims=True)

    def row_of(both):
        return jnp.sum(both.T, axis=0, keepdims=True)

    def factor_rows(row, count):
        mean = row / jnp.maximum(count, 1.0)
        other = pltpu.roll(mean, WINDOW, 1)
        scale = 1.0 / jnp.sqrt(jnp.maximum(mean - other * other, 0.0) + 0.1)
        lane = lax.broadcasted_iota(jnp.int32, row.shape, 1)
        return jnp.where(lane < WINDOW, mean, scale)

    def upright(row):
        return jnp.broadcast_to(row, (LANES, LANES)).T


    def roll_window(f, b, place):
        top = pl.multiple_of(b * WINDOW, WINDOW)

        def chunk(c, carry):
            cols = columns(c)
            reach = pl.ds(top, 2 * WINDOW)
            sums = x[f, reach, cols] * weight[reach, cols]
            for step in (8, 16, 32):
                sums = sums[step:] + sums[:-step]
            for step in (1, 2, 4):
                sums = sums + pltpu.roll(sums, step, 0)
            means = sums[8:] * inverse[pl.ds(top + WINDOW, WINDOW), cols]
            rolling[f, pl.ds(top, WINDOW), cols] = means
            return carry[0] + means, carry[1] + means * means

        total, square = lax.fori_loop(0, chunks, chunk, (zero, zero), unroll=UNROLL)
        place[:WINDOW] = total
        place[WINDOW:] = square

    def clip_scores(f, b, tall, place):
        top = pl.multiple_of(b * WINDOW, WINDOW)
        center, scale = tall[:WINDOW], tall[WINDOW:]

        def chunk(c, carry):
            cols = columns(c)
            here = pl.ds(top, WINDOW)
            scored = (rolling[f, here, cols] - center) * scale
            clipped = jnp.minimum(jnp.maximum(scored, -CLIP), CLIP)
            rolling[f, here, cols] = clipped
            masked = clipped * weight[pl.ds(top + WINDOW, WINDOW), cols]
            return carry[0] + masked, carry[1] + masked * clipped

        total, square = lax.fori_loop(0, chunks, chunk, (zero, zero), unroll=UNROLL)
        place[:WINDOW] = total
        place[WINDOW:] = square

    def finish(f, b, tall, target, base):
        top = pl.multiple_of(b * WINDOW, WINDOW)
        base = pl.multiple_of(base, WINDOW)
        middle, factor = tall[:WINDOW], tall[WINDOW:]

        @pl.loop(0, chunks, unroll=UNROLL)
        def chunk(c):
            cols = columns(c)
            clipped = rolling[f, pl.ds(top, WINDOW), cols]
            deviate = (clipped - middle) * weight[pl.ds(top + WINDOW, WINDOW), cols]
            target[pl.ds(base, WINDOW), cols] = deviate * factor

    def places(g):
        start, size = groups[g]
        number = size * (blocks - 1)
        where = [(start + i % size, 1 + i // size) for i in range(number)]
        if start + size == fields:
            where.append((ahead, 0))
        return where

    def items(g):
        start, size = groups[g]
        whole = size * (blocks - 1)
        if start + size < fields:
            return whole, lambda i: (start + lax.rem(i, size), 1 + lax.div(i, size))
        return whole + is_first.astype(jnp.int32), lambda i: (
            jnp.where(i < whole, start + lax.rem(i, size), ahead),
            jnp.where(i < whole, 1 + lax.div(i, size), 0),
        )

    def gather_rows(g, slot):
        for i in range(len(places(g))):
            part[slot, pl.ds(i, 1), :] = row_of(lanes[1 + g, i])
        send(slot)

    def spread_rows(g, slot):
        total = receive(slot)
        number = len(places(g))
        count = jnp.concatenate([totals[pl.ds(b, 1), :] for _, b in places(g)], axis=0)
        rows_of = factor_rows(total[:number], count)
        for i in range(number):
            spread[g, i] = upright(rows_of[i : i + 1])

    def meet_plane():
        for i in range(blocks + 1):
            part[0, pl.ds(i, 1), :] = row_of(lanes[0, i])
        pl.semaphore_wait(ready, len(cross_peers))
        send(0)

    def main_first(g):
        start, size = groups[g]
        for f in range(start, start + size):
            loads[f].wait()
        number, place = items(g)

        @pl.loop(0, number)
        def item(i):
            f, b = place(i)
            roll_window(f, b, lanes.at[1 + g, i])

        if g == 0:
            meet_plane()
        gather_rows(g, 1 + 2 * g)

    def main_second(g):
        spread_rows(g, 1 + 2 * g)
        number, place = items(g)

        @pl.loop(0, number)
        def item(i):
            f, b = place(i)
            clip_scores(f, b, spread[g, i], lanes.at[1 + g, i])

        gather_rows(g, 2 + 2 * g)

    def main_third(g):
        spread_rows(g, 2 + 2 * g)
        number, place = items(g)

        @pl.loop(0, number)
        def item(i):
            f, b = place(i)
            finish(f, b, spread[g, i], out.at[f], b * WINDOW)

    single = lanes.at[0, 0]

    def tail_first(f, b):
        roll_window(f, b, single)
        tail_part[2 * f] = row_of(single[...])
        send_row(2 * f)

    def tail_factors(slot, b):
        return upright(factor_rows(receive_row(slot), totals[pl.ds(b, 1), :]))

    def tail_second(f, b):
        clip_scores(f, b, tail_factors(2 * f, b), single)
        tail_part[2 * f + 1] = row_of(single[...])
        send_row(2 * f + 1)

    def tail_third(f, b, target):
        finish(f, b, tail_factors(2 * f + 1, b), target, 0)

    def ahead_first():
        upcoming.wait_recv()
        tail_first(ahead, blocks)

    def ahead_second():
        tail_second(ahead, blocks)

    def ahead_third():
        tail_third(ahead, blocks, stage)
        finished.start()

    not_last = pl.when(jnp.logical_not(is_last))

    def relay(copy):
        def pass_on():
            copy[0].wait_recv()
            copy[1].start()

        return pass_on

    def first(f):
        halos[f].wait_recv()
        if f == ahead - 1:
            pl.when(jnp.logical_not(is_first))(cross_onward.wait_recv)
        tail_first(f, 0)

    def second(f):
        tail_second(f, 0)

    def third(f):
        tail_third(f, 0, out.at[f])

    main_first(0)
    main_first(1)
    totals[...] = receive(0)
    main_second(0)
    not_last(ahead_first)
    first(0)
    main_second(1)
    pl.when(is_last)(relay((even_detour, cross_onward)))
    main_third(0)
    not_last(ahead_second)
    pl.when(tm == 1)(relay((even_detour, cross_onward)))
    pl.when(is_last)(relay((odd_detour, back_onward)))
    second(0)
    main_third(1)
    first(1)
    not_last(ahead_third)
    third(0)
    first(2)
    second(1)
    second(2)
    third(1)
    third(2)

    @pl.when(jnp.logical_not(is_first))
    def arrivals():
        finished.wait_recv()
        upcoming.wait_send()

    pl.when(jnp.logical_not(is_last))(even_detour.wait_send)
    pl.when(jnp.logical_not(is_even))(cross_onward.wait_send)
    pl.when(is_last)(back_onward.wait_send)
    for copy in halos:
        copy.wait_send()
    for slot in range(part.shape[0]):
        sent = got.at[slot]
        pltpu.make_async_copy(sent, sent, send_sem.at[slot]).wait()

    def row_sent(slot):
        sent = tail_got.at[slot]
        pltpu.make_async_copy(sent, sent, tail_send.at[slot]).wait()

    for slot in range(2 * ahead):
        row_sent(slot)

    @not_last
    def departures():
        finished.wait_send()
        row_sent(2 * ahead)
        row_sent(2 * ahead + 1)


def per_device(n_tm, n_as, values, listed_from, listed_until):
    fields, rows, assets = values.shape
    blocks = rows // WINDOW
    groups = field_groups(fields)
    stats = -(-max(groups[0][1] * (blocks - 1) + 1, blocks + 2) // 8) * 8
    slots = 1 + 2 * len(groups)
    f32 = jnp.float32
    vmem = pltpu.VMEM
    dma = pltpu.SemaphoreType.DMA
    return pl.pallas_call(
        functools.partial(kernel, n_tm, n_as),
        out_shape=vmem((fields, rows, assets), f32),
        in_specs=[pl.BlockSpec(memory_space=pltpu.HBM)] * 3,
        out_specs=pl.BlockSpec(memory_space=vmem),
        scratch_shapes=[
            vmem((fields, rows + 2 * WINDOW, assets), f32),
            vmem((fields, rows + WINDOW, assets), f32),
            vmem((rows + 2 * WINDOW, assets), f32),
            vmem((rows + 2 * WINDOW, assets), f32),
            vmem((1, assets), jnp.int32),
            vmem((1, assets), jnp.int32),
            vmem((WINDOW, assets), f32),
            vmem((2, WINDOW, assets - DIRECT), f32),
            vmem((1 + len(groups), stats, LANES, LANES), f32),
            vmem((len(groups), stats, LANES, LANES), f32),
            vmem((slots, stats, LANES), f32),
            vmem((slots, n_as - 1, stats, LANES), f32),
            vmem((stats, LANES), f32),
            vmem((2 * fields, 1, LANES), f32),
            vmem((2 * fields, n_as - 1, LANES), f32),
            dma((fields + 2,)),
            dma((fields,)),
            dma((fields,)),
            dma((2,)),
            dma((2,)),
            dma((1,)),
            dma((2,)),
            dma((2,)),
            dma((1,)),
            pltpu.SemaphoreType.REGULAR,
            dma((slots,)),
            dma((slots,)),
            dma((2 * fields,)),
            dma((2 * fields,)),
        ],
        compiler_params=pltpu.CompilerParams(
            collective_id=0, has_side_effects=True, vmem_limit_bytes=48 * 2**20
        ),
    )(values, listed_from[None], listed_until[None])


def solution(mesh):
    in_specs = (P(None, "tm", "asset"), P("asset"), P("asset"))
    out_specs = P(None, "tm", "asset")
    body = functools.partial(per_device, mesh.shape["tm"], mesh.shape["asset"])
    return jax.shard_map(
        body, mesh=mesh, in_specs=in_specs, out_specs=out_specs, check_vma=False
    )
```

```python
import functools

import jax
import jax.numpy as jnp
from jax import lax
from jax.experimental import pallas as pl
from jax.experimental.pallas import tpu as pltpu
from jax.sharding import PartitionSpec as P

WINDOW = 64
LANES = 128
CLIP = 3.0
UNROLL = 4
LINE = 8
DIRECT = 1024
PIECES = 2


def field_groups(fields):
    half = (fields + 1) // 2
    return [(start, min(half, fields - start)) for start in range(0, fields, half)]


def plane(n_as, me):
    lines, width = n_as // LINE, LINE // 2
    steps = [(i, j, k) for i in range(lines) for j in range(width) for k in range(2)]
    steps = [step for step in steps if step != (0, 0, 0)]
    steps.sort(key=lambda s: -min(s[0], lines - s[0]) - min(s[1], width - s[1]))
    row, column, core = lax.div(me, LINE), lax.rem(lax.div(me, 2), width), lax.rem(me, 2)
    return [
        lax.rem(row + i, lines) * LINE + lax.rem(column + j, width) * 2 + lax.rem(core + k, 2)
        for i, j, k in steps
    ]


def kernel(
    n_tm, n_as, values, opened_hbm, closed_hbm, out,
    x, rolling, weight, inverse, opened_ref, closed_ref, stage, hold, lanes, spread,
    part, got, totals, tail_part, tail_got,
    load_sem, halo_send, halo_recv, next_sem, done_sem, hold_send, hold_recv, late_send, late_recv, ready,
    send_sem, recv_sem, tail_send, tail_recv,
):
    fields, rows, assets = values.shape
    blocks = rows // WINDOW
    chunks = assets // LANES
    groups = field_groups(fields)
    ahead = fields - 1
    tm = lax.axis_index("tm")
    me = lax.axis_index("asset")
    later = lax.rem(tm + 1, n_tm)
    before = lax.rem(tm + n_tm - 1, n_tm)
    across = lax.rem(tm + 2, n_tm)
    is_first = tm == 0
    is_last = tm == n_tm - 1
    spot = lax.rem(me, LINE)
    line_peers = [me - spot + lax.rem(spot + d, LINE) for d in range(1, LINE)]
    cross_peers = [lax.rem(me + LINE * d, n_as) for d in range(1, n_as // LINE)]
    plane_peers = plane(n_as, me)

    dates = [
        pltpu.make_async_copy(opened_hbm, opened_ref, load_sem.at[fields]),
        pltpu.make_async_copy(closed_hbm, closed_ref, load_sem.at[fields + 1]),
    ]
    loads = [
        pltpu.make_async_copy(values.at[f], x.at[f, pl.ds(WINDOW, rows)], load_sem.at[f])
        for f in range(fields)
    ]

    barrier = pltpu.get_barrier_semaphore()
    for other in (later, before, across):
        pl.semaphore_signal(barrier, inc=1, device_id={"tm": other})
    for other in line_peers + cross_peers:
        pl.semaphore_signal(barrier, inc=1, device_id={"asset": other})
    for copy in dates + loads:
        copy.start()

    def columns(c):
        return pl.ds(pl.multiple_of(c * LANES, LANES), LANES)

    zero = jnp.zeros((WINDOW, LANES), jnp.float32)
    part[...] = jnp.zeros(part.shape, part.dtype)
    lanes[...] = jnp.zeros(lanes.shape, lanes.dtype)

    @pl.when(is_first)
    def no_past():
        for f in range(fields):
            x[f, :WINDOW, :] = jnp.zeros((WINDOW, assets), jnp.float32)

    first_stamp = tm * rows - WINDOW
    for copy in dates:
        copy.wait()

    pl.semaphore_wait(barrier, 3 + len(line_peers) + len(cross_peers))

    past = pl.ds(rows - WINDOW, WINDOW)
    pieces = [(f, 0, assets) for f in range(ahead - 1)]
    pieces += [(ahead - 1, start, DIRECT // PIECES) for start in range(0, DIRECT, DIRECT // PIECES)]
    rest = pl.ds(DIRECT, assets - DIRECT)
    halos = [
        pltpu.make_async_remote_copy(
            src_ref=values.at[f, past, pl.ds(start, width)],
            dst_ref=x.at[f, pl.ds(0, WINDOW), pl.ds(start, width)],
            send_sem=halo_send.at[k],
            recv_sem=halo_recv.at[k],
            device_id={"tm": later},
        )
        for k, (f, start, width) in enumerate(pieces)
    ]
    upcoming = pltpu.make_async_remote_copy(
        src_ref=values.at[ahead, pl.ds(0, WINDOW)],
        dst_ref=x.at[ahead, pl.ds(WINDOW + rows, WINDOW)],
        send_sem=next_sem.at[0],
        recv_sem=next_sem.at[1],
        device_id={"tm": before},
    )
    finished = pltpu.make_async_remote_copy(
        src_ref=stage,
        dst_ref=out.at[ahead, pl.ds(0, WINDOW)],
        send_sem=done_sem.at[0],
        recv_sem=done_sem.at[1],
        device_id={"tm": later},
    )

    def detour(slot, other):
        return pltpu.make_async_remote_copy(
            src_ref=values.at[ahead - 1, past, rest],
            dst_ref=hold.at[slot],
            send_sem=hold_send.at[0],
            recv_sem=hold_recv.at[slot],
            device_id={"tm": other},
        )

    def onward(slot, other):
        return pltpu.make_async_remote_copy(
            src_ref=hold.at[slot],
            dst_ref=x.at[ahead - 1, pl.ds(0, WINDOW), rest],
            send_sem=late_send.at[slot],
            recv_sem=late_recv.at[0],
            device_id={"tm": other},
        )

    is_even = lax.rem(tm, 2) == 0
    even_detour, odd_detour = detour(0, before), detour(1, across)
    cross_onward, back_onward = onward(0, across), onward(1, before)

    pl.when(jnp.logical_not(is_first))(upcoming.start)
    pl.when(is_even)(even_detour.start)
    pl.when(tm == 1)(odd_detour.start)
    for copy in halos:
        pl.when(jnp.logical_not(is_last))(copy.start)
    for other in cross_peers:
        pl.semaphore_signal(ready, inc=1, device_id={"asset": other})

    @pl.loop(0, blocks + 2)
    def listing(b):
        start = pl.multiple_of(b * WINDOW, WINDOW)
        stamps = first_stamp + start + lax.broadcasted_iota(jnp.int32, (WINDOW, LANES), 0)

        def chunk(c, total):
            cols = columns(c)
            opened = jnp.maximum(opened_ref[:, cols], 0)
            closed = closed_ref[:, cols]
            listed = (stamps >= opened) & (stamps < closed)
            low = jnp.maximum(stamps - (WINDOW - 1), opened)
            counted = jnp.maximum(jnp.minimum(stamps + 1, closed) - low, 1).astype(jnp.float32)
            ones = jnp.where(listed, 1.0, 0.0)
            weight[pl.ds(start, WINDOW), cols] = ones
            inverse[pl.ds(start, WINDOW), cols] = ones / counted
            return total + ones

        total = lax.fori_loop(0, chunks, chunk, zero, unroll=2)
        here = lax.rem(b + blocks + 1, blocks + 2)
        lanes[0, here, :WINDOW] = total
        lanes[0, here, WINDOW:] = total

    def send(slot):
        for d, other in enumerate(plane_peers):
            pltpu.make_async_remote_copy(
                src_ref=part.at[slot],
                dst_ref=got.at[slot, d],
                send_sem=send_sem.at[slot],
                recv_sem=recv_sem.at[slot],
                device_id={"asset": other},
            ).start()

    def receive(slot):
        arrived = got.at[slot]
        pltpu.make_async_copy(arrived, arrived, recv_sem.at[slot]).wait()
        return part[slot] + jnp.sum(got[slot], axis=0)

    def send_row(slot):
        for d, other in enumerate(plane_peers):
            pltpu.make_async_remote_copy(
                src_ref=tail_part.at[slot],
                dst_ref=tail_got.at[slot, pl.ds(d, 1)],
                send_sem=tail_send.at[slot],
                recv_sem=tail_recv.at[slot],
                device_id={"asset": other},
            ).start()

    def receive_row(slot):
        arrived = tail_got.at[slot]
        pltpu.make_async_copy(arrived, arrived, tail_recv.at[slot]).wait()
        return tail_part[slot] + jnp.sum(tail_got[slot], axis=0, keepdims=True)

    def row_of(both):
        return jnp.sum(both.T, axis=0, keepdims=True)

    def factor_rows(row, count):
        mean = row / jnp.maximum(count, 1.0)
        other = pltpu.roll(mean, WINDOW, 1)
        scale = 1.0 / jnp.sqrt(jnp.maximum(mean - other * other, 0.0) + 0.1)
        lane = lax.broadcasted_iota(jnp.int32, row.shape, 1)
        return jnp.where(lane < WINDOW, mean, scale)

    def upright(row):
        return jnp.broadcast_to(row, (LANES, LANES)).T


    def roll_window(f, b, place, start=0, stop=chunks, begin=(zero, zero)):
        top = pl.multiple_of(b * WINDOW, WINDOW)

        def chunk(c, carry):
            cols = columns(c)
            reach = pl.ds(top, 2 * WINDOW)
            sums = x[f, reach, cols] * weight[reach, cols]
            for step in (8, 16, 32):
                sums = sums[step:] + sums[:-step]
            for step in (1, 2, 4):
                sums = sums + pltpu.roll(sums, step, 0)
            means = sums[8:] * inverse[pl.ds(top + WINDOW, WINDOW), cols]
            rolling[f, pl.ds(top, WINDOW), cols] = means
            return carry[0] + means, carry[1] + means * means

        total, square = lax.fori_loop(start, stop, chunk, begin, unroll=UNROLL)
        place[:WINDOW] = total
        place[WINDOW:] = square

    def clip_scores(f, b, tall, place):
        top = pl.multiple_of(b * WINDOW, WINDOW)
        center, scale = tall[:WINDOW], tall[WINDOW:]

        def chunk(c, carry):
            cols = columns(c)
            here = pl.ds(top, WINDOW)
            scored = (rolling[f, here, cols] - center) * scale
            clipped = jnp.minimum(jnp.maximum(scored, -CLIP), CLIP)
            rolling[f, here, cols] = clipped
            masked = clipped * weight[pl.ds(top + WINDOW, WINDOW), cols]
            return carry[0] + masked, carry[1] + masked * clipped

        total, square = lax.fori_loop(0, chunks, chunk, (zero, zero), unroll=UNROLL)
        place[:WINDOW] = total
        place[WINDOW:] = square

    def finish(f, b, tall, target, base):
        top = pl.multiple_of(b * WINDOW, WINDOW)
        base = pl.multiple_of(base, WINDOW)
        middle, factor = tall[:WINDOW], tall[WINDOW:]

        @pl.loop(0, chunks, unroll=UNROLL)
        def chunk(c):
            cols = columns(c)
            clipped = rolling[f, pl.ds(top, WINDOW), cols]
            deviate = (clipped - middle) * weight[pl.ds(top + WINDOW, WINDOW), cols]
            target[pl.ds(base, WINDOW), cols] = deviate * factor

    def places(g):
        start, size = groups[g]
        number = size * (blocks - 1)
        where = [(start + i % size, 1 + i // size) for i in range(number)]
        if start + size == fields:
            where.append((ahead, 0))
        return where

    def items(g):
        start, size = groups[g]
        whole = size * (blocks - 1)
        if start + size < fields:
            return whole, lambda i: (start + lax.rem(i, size), 1 + lax.div(i, size))
        return whole + is_first.astype(jnp.int32), lambda i: (
            jnp.where(i < whole, start + lax.rem(i, size), ahead),
            jnp.where(i < whole, 1 + lax.div(i, size), 0),
        )

    def gather_rows(g, slot):
        for i in range(len(places(g))):
            part[slot, pl.ds(i, 1), :] = row_of(lanes[1 + g, i])
        send(slot)

    def spread_rows(g, slot):
        total = receive(slot)
        number = len(places(g))
        count = jnp.concatenate([totals[pl.ds(b, 1), :] for _, b in places(g)], axis=0)
        rows_of = factor_rows(total[:number], count)
        for i in range(number):
            spread[g, i] = upright(rows_of[i : i + 1])

    def meet_plane():
        for i in range(blocks + 1):
            part[0, pl.ds(i, 1), :] = row_of(lanes[0, i])
        pl.semaphore_wait(ready, len(cross_peers))
        send(0)

    def main_first(g):
        start, size = groups[g]
        for f in range(start, start + size):
            loads[f].wait()
        number, place = items(g)

        @pl.loop(0, number)
        def item(i):
            f, b = place(i)
            roll_window(f, b, lanes.at[1 + g, i])

        if g == 0:
            meet_plane()
        gather_rows(g, 1 + 2 * g)

    def main_second(g):
        spread_rows(g, 1 + 2 * g)
        number, place = items(g)

        @pl.loop(0, number)
        def item(i):
            f, b = place(i)
            clip_scores(f, b, spread[g, i], lanes.at[1 + g, i])

        gather_rows(g, 2 + 2 * g)

    def main_third(g):
        spread_rows(g, 2 + 2 * g)
        number, place = items(g)

        @pl.loop(0, number)
        def item(i):
            f, b = place(i)
            finish(f, b, spread[g, i], out.at[f], b * WINDOW)

    single = lanes.at[0, 0]

    def tail_first(f, b):
        roll_window(f, b, single)
        tail_part[2 * f] = row_of(single[...])
        send_row(2 * f)

    def tail_factors(slot, b):
        return upright(factor_rows(receive_row(slot), totals[pl.ds(b, 1), :]))

    def tail_second(f, b):
        clip_scores(f, b, tail_factors(2 * f, b), single)
        tail_part[2 * f + 1] = row_of(single[...])
        send_row(2 * f + 1)

    def tail_third(f, b, target):
        finish(f, b, tail_factors(2 * f + 1, b), target, 0)

    def ahead_first():
        upcoming.wait_recv()
        tail_first(ahead, blocks)

    def ahead_second():
        tail_second(ahead, blocks)

    def ahead_third():
        tail_third(ahead, blocks, stage)
        finished.start()

    not_last = pl.when(jnp.logical_not(is_last))

    def relay(copy):
        def pass_on():
            copy[0].wait_recv()
            copy[1].start()

        return pass_on

    def first(f):
        waits = [(halos[k].wait_recv, start, width) for k, (g, start, width) in enumerate(pieces) if g == f]
        if f == ahead - 1:
            waits.insert(0, (cross_onward.wait_recv, DIRECT, assets - DIRECT))
        begin = (zero, zero)
        for wait, start, width in waits:
            pl.when(jnp.logical_not(is_first))(wait)
            roll_window(f, 0, single, start // LANES, (start + width) // LANES, begin)
            begin = (single[:WINDOW], single[WINDOW:])
        tail_part[2 * f] = row_of(single[...])
        send_row(2 * f)

    def second(f):
        tail_second(f, 0)

    def third(f):
        tail_third(f, 0, out.at[f])

    main_first(0)
    main_first(1)
    totals[...] = receive(0)
    main_second(0)
    not_last(ahead_first)
    first(0)
    main_second(1)
    pl.when(is_last)(relay((even_detour, cross_onward)))
    main_third(0)
    not_last(ahead_second)
    pl.when(tm == 1)(relay((even_detour, cross_onward)))
    pl.when(is_last)(relay((odd_detour, back_onward)))
    second(0)
    main_third(1)
    first(1)
    not_last(ahead_third)
    third(0)
    first(2)
    second(1)
    second(2)
    third(1)
    third(2)

    @pl.when(jnp.logical_not(is_first))
    def arrivals():
        finished.wait_recv()
        upcoming.wait_send()

    pl.when(jnp.logical_not(is_last))(even_detour.wait_send)
    pl.when(jnp.logical_not(is_even))(cross_onward.wait_send)
    pl.when(is_last)(back_onward.wait_send)
    for copy in halos:
        pl.when(jnp.logical_not(is_last))(copy.wait_send)
    for slot in range(part.shape[0]):
        sent = got.at[slot]
        pltpu.make_async_copy(sent, sent, send_sem.at[slot]).wait()

    def row_sent(slot):
        sent = tail_got.at[slot]
        pltpu.make_async_copy(sent, sent, tail_send.at[slot]).wait()

    for slot in range(2 * ahead):
        row_sent(slot)

    @not_last
    def departures():
        finished.wait_send()
        row_sent(2 * ahead)
        row_sent(2 * ahead + 1)


def per_device(n_tm, n_as, values, listed_from, listed_until):
    fields, rows, assets = values.shape
    blocks = rows // WINDOW
    groups = field_groups(fields)
    stats = -(-max(groups[0][1] * (blocks - 1) + 1, blocks + 2) // 8) * 8
    slots = 1 + 2 * len(groups)
    f32 = jnp.float32
    vmem = pltpu.VMEM
    dma = pltpu.SemaphoreType.DMA
    return pl.pallas_call(
        functools.partial(kernel, n_tm, n_as),
        out_shape=vmem((fields, rows, assets), f32),
        in_specs=[pl.BlockSpec(memory_space=pltpu.HBM)] * 3,
        out_specs=pl.BlockSpec(memory_space=vmem),
        scratch_shapes=[
            vmem((fields, rows + 2 * WINDOW, assets), f32),
            vmem((fields, rows + WINDOW, assets), f32),
            vmem((rows + 2 * WINDOW, assets), f32),
            vmem((rows + 2 * WINDOW, assets), f32),
            vmem((1, assets), jnp.int32),
            vmem((1, assets), jnp.int32),
            vmem((WINDOW, assets), f32),
            vmem((2, WINDOW, assets - DIRECT), f32),
            vmem((1 + len(groups), stats, LANES, LANES), f32),
            vmem((len(groups), stats, LANES, LANES), f32),
            vmem((slots, stats, LANES), f32),
            vmem((slots, n_as - 1, stats, LANES), f32),
            vmem((stats, LANES), f32),
            vmem((2 * fields, 1, LANES), f32),
            vmem((2 * fields, n_as - 1, LANES), f32),
            dma((fields + 2,)),
            dma((fields - 2 + PIECES,)),
            dma((fields - 2 + PIECES,)),
            dma((2,)),
            dma((2,)),
            dma((1,)),
            dma((2,)),
            dma((2,)),
            dma((1,)),
            pltpu.SemaphoreType.REGULAR,
            dma((slots,)),
            dma((slots,)),
            dma((2 * fields,)),
            dma((2 * fields,)),
        ],
        compiler_params=pltpu.CompilerParams(
            collective_id=0, has_side_effects=True, vmem_limit_bytes=48 * 2**20
        ),
    )(values, listed_from[None], listed_until[None])


def solution(mesh):
    in_specs = (P(None, "tm", "asset"), P("asset"), P("asset"))
    out_specs = P(None, "tm", "asset")
    body = functools.partial(per_device, mesh.shape["tm"], mesh.shape["asset"])
    return jax.shard_map(
        body, mesh=mesh, in_specs=in_specs, out_specs=out_specs, check_vma=False
    )
```

```python
import functools

import jax
import jax.numpy as jnp
from jax import lax
from jax.experimental import pallas as pl
from jax.experimental.pallas import tpu as pltpu
from jax.sharding import PartitionSpec as P

WINDOW = 64
LANES = 128
CLIP = 3.0
UNROLL = 4
LINE = 8
DIRECT = 896
PIECES = 7
RELAYS = 3


def field_groups(fields):
    half = (fields + 1) // 2
    return [(start, min(half, fields - start)) for start in range(0, fields, half)]


def plane(n_as, me):
    lines, width = n_as // LINE, LINE // 2
    steps = [(i, j, k) for i in range(lines) for j in range(width) for k in range(2)]
    steps = [step for step in steps if step != (0, 0, 0)]
    steps.sort(key=lambda s: -min(s[0], lines - s[0]) - min(s[1], width - s[1]))
    row, column, core = lax.div(me, LINE), lax.rem(lax.div(me, 2), width), lax.rem(me, 2)
    return [
        lax.rem(row + i, lines) * LINE + lax.rem(column + j, width) * 2 + lax.rem(core + k, 2)
        for i, j, k in steps
    ]


def kernel(
    n_tm, n_as, values, opened_hbm, closed_hbm, out,
    x, rolling, weight, inverse, opened_ref, closed_ref, stage, hold, lanes, spread,
    part, got, totals, tail_part, tail_got,
    load_sem, halo_send, halo_recv, next_sem, done_sem, hold_send, hold_recv, late_send, late_recv, ready,
    send_sem, recv_sem, tail_send, tail_recv,
):
    fields, rows, assets = values.shape
    blocks = rows // WINDOW
    chunks = assets // LANES
    groups = field_groups(fields)
    ahead = fields - 1
    tm = lax.axis_index("tm")
    me = lax.axis_index("asset")
    later = lax.rem(tm + 1, n_tm)
    before = lax.rem(tm + n_tm - 1, n_tm)
    across = lax.rem(tm + 2, n_tm)
    is_first = tm == 0
    is_last = tm == n_tm - 1
    spot = lax.rem(me, LINE)
    line_peers = [me - spot + lax.rem(spot + d, LINE) for d in range(1, LINE)]
    cross_peers = [lax.rem(me + LINE * d, n_as) for d in range(1, n_as // LINE)]
    plane_peers = plane(n_as, me)

    dates = [
        pltpu.make_async_copy(opened_hbm, opened_ref, load_sem.at[fields]),
        pltpu.make_async_copy(closed_hbm, closed_ref, load_sem.at[fields + 1]),
    ]
    loads = [
        pltpu.make_async_copy(values.at[f], x.at[f, pl.ds(WINDOW, rows)], load_sem.at[f])
        for f in range(fields)
    ]

    barrier = pltpu.get_barrier_semaphore()
    for other in (later, before, across):
        pl.semaphore_signal(barrier, inc=1, device_id={"tm": other})
    for other in line_peers + cross_peers:
        pl.semaphore_signal(barrier, inc=1, device_id={"asset": other})
    for copy in dates + loads:
        copy.start()

    def columns(c):
        return pl.ds(pl.multiple_of(c * LANES, LANES), LANES)

    zero = jnp.zeros((WINDOW, LANES), jnp.float32)
    part[...] = jnp.zeros(part.shape, part.dtype)
    lanes[...] = jnp.zeros(lanes.shape, lanes.dtype)

    @pl.when(is_first)
    def no_past():
        for f in range(fields):
            x[f, :WINDOW, :] = jnp.zeros((WINDOW, assets), jnp.float32)

    first_stamp = tm * rows - WINDOW
    for copy in dates:
        copy.wait()

    pl.semaphore_wait(barrier, 3 + len(line_peers) + len(cross_peers))

    past = pl.ds(rows - WINDOW, WINDOW)
    pieces = [(f, 0, assets) for f in range(ahead - 1)]
    pieces += [(ahead - 1, start, DIRECT // PIECES) for start in range(0, DIRECT, DIRECT // PIECES)]
    share = (assets - DIRECT) // RELAYS
    rest = [pl.ds(DIRECT + k * share, share) for k in range(RELAYS)]
    halos = [
        pltpu.make_async_remote_copy(
            src_ref=values.at[f, past, pl.ds(start, width)],
            dst_ref=x.at[f, pl.ds(0, WINDOW), pl.ds(start, width)],
            send_sem=halo_send.at[k],
            recv_sem=halo_recv.at[k],
            device_id={"tm": later},
        )
        for k, (f, start, width) in enumerate(pieces)
    ]
    upcoming = pltpu.make_async_remote_copy(
        src_ref=values.at[ahead, pl.ds(0, WINDOW)],
        dst_ref=x.at[ahead, pl.ds(WINDOW + rows, WINDOW)],
        send_sem=next_sem.at[0],
        recv_sem=next_sem.at[1],
        device_id={"tm": before},
    )
    finished = pltpu.make_async_remote_copy(
        src_ref=stage,
        dst_ref=out.at[ahead, pl.ds(0, WINDOW)],
        send_sem=done_sem.at[0],
        recv_sem=done_sem.at[1],
        device_id={"tm": later},
    )

    def detour(slot, other):
        return [
            pltpu.make_async_remote_copy(
                src_ref=values.at[ahead - 1, past, rest[k]],
                dst_ref=hold.at[slot, k],
                send_sem=hold_send.at[k],
                recv_sem=hold_recv.at[slot, k],
                device_id={"tm": other},
            )
            for k in range(RELAYS)
        ]

    def onward(slot, other):
        return [
            pltpu.make_async_remote_copy(
                src_ref=hold.at[slot, k],
                dst_ref=x.at[ahead - 1, pl.ds(0, WINDOW), rest[k]],
                send_sem=late_send.at[slot, k],
                recv_sem=late_recv.at[k],
                device_id={"tm": other},
            )
            for k in range(RELAYS)
        ]

    is_even = lax.rem(tm, 2) == 0
    even_detour, odd_detour = detour(0, before), detour(1, across)
    cross_onward, back_onward = onward(0, across), onward(1, before)

    pl.when(jnp.logical_not(is_first))(upcoming.start)
    for k in range(RELAYS):
        pl.when(is_even)(even_detour[k].start)
        pl.when(tm == 1)(odd_detour[k].start)
    for copy in halos:
        pl.when(jnp.logical_not(is_last))(copy.start)
    for other in cross_peers:
        pl.semaphore_signal(ready, inc=1, device_id={"asset": other})

    @pl.loop(0, blocks + 2)
    def listing(b):
        start = pl.multiple_of(b * WINDOW, WINDOW)
        stamps = first_stamp + start + lax.broadcasted_iota(jnp.int32, (WINDOW, LANES), 0)

        def chunk(c, total):
            cols = columns(c)
            opened = jnp.maximum(opened_ref[:, cols], 0)
            closed = closed_ref[:, cols]
            listed = (stamps >= opened) & (stamps < closed)
            low = jnp.maximum(stamps - (WINDOW - 1), opened)
            counted = jnp.maximum(jnp.minimum(stamps + 1, closed) - low, 1).astype(jnp.float32)
            ones = jnp.where(listed, 1.0, 0.0)
            weight[pl.ds(start, WINDOW), cols] = ones
            inverse[pl.ds(start, WINDOW), cols] = ones / counted
            return total + ones

        total = lax.fori_loop(0, chunks, chunk, zero, unroll=2)
        here = lax.rem(b + blocks + 1, blocks + 2)
        lanes[0, here, :WINDOW] = total
        lanes[0, here, WINDOW:] = total

    def send(slot):
        for d, other in enumerate(plane_peers):
            pltpu.make_async_remote_copy(
                src_ref=part.at[slot],
                dst_ref=got.at[slot, d],
                send_sem=send_sem.at[slot],
                recv_sem=recv_sem.at[slot],
                device_id={"asset": other},
            ).start()

    def receive(slot):
        arrived = got.at[slot]
        pltpu.make_async_copy(arrived, arrived, recv_sem.at[slot]).wait()
        return part[slot] + jnp.sum(got[slot], axis=0)

    def send_row(slot):
        for d, other in enumerate(plane_peers):
            pltpu.make_async_remote_copy(
                src_ref=tail_part.at[slot],
                dst_ref=tail_got.at[slot, pl.ds(d, 1)],
                send_sem=tail_send.at[slot],
                recv_sem=tail_recv.at[slot],
                device_id={"asset": other},
            ).start()

    def receive_row(slot):
        arrived = tail_got.at[slot]
        pltpu.make_async_copy(arrived, arrived, tail_recv.at[slot]).wait()
        return tail_part[slot] + jnp.sum(tail_got[slot], axis=0, keepdims=True)

    def row_of(both):
        return jnp.sum(both.T, axis=0, keepdims=True)

    def factor_rows(row, count):
        mean = row / jnp.maximum(count, 1.0)
        other = pltpu.roll(mean, WINDOW, 1)
        scale = 1.0 / jnp.sqrt(jnp.maximum(mean - other * other, 0.0) + 0.1)
        lane = lax.broadcasted_iota(jnp.int32, row.shape, 1)
        return jnp.where(lane < WINDOW, mean, scale)

    def upright(row):
        return jnp.broadcast_to(row, (LANES, LANES)).T


    def roll_window(f, b, place, start=0, stop=chunks, begin=(zero, zero)):
        top = pl.multiple_of(b * WINDOW, WINDOW)

        def chunk(c, carry):
            cols = columns(c)
            reach = pl.ds(top, 2 * WINDOW)
            sums = x[f, reach, cols] * weight[reach, cols]
            for step in (8, 16, 32):
                sums = sums[step:] + sums[:-step]
            for step in (1, 2, 4):
                sums = sums + pltpu.roll(sums, step, 0)
            means = sums[8:] * inverse[pl.ds(top + WINDOW, WINDOW), cols]
            rolling[f, pl.ds(top, WINDOW), cols] = means
            return carry[0] + means, carry[1] + means * means

        total, square = lax.fori_loop(start, stop, chunk, begin, unroll=UNROLL)
        place[:WINDOW] = total
        place[WINDOW:] = square

    def clip_scores(f, b, tall, place):
        top = pl.multiple_of(b * WINDOW, WINDOW)
        center, scale = tall[:WINDOW], tall[WINDOW:]

        def chunk(c, carry):
            cols = columns(c)
            here = pl.ds(top, WINDOW)
            scored = (rolling[f, here, cols] - center) * scale
            clipped = jnp.minimum(jnp.maximum(scored, -CLIP), CLIP)
            rolling[f, here, cols] = clipped
            masked = clipped * weight[pl.ds(top + WINDOW, WINDOW), cols]
            return carry[0] + masked, carry[1] + masked * clipped

        total, square = lax.fori_loop(0, chunks, chunk, (zero, zero), unroll=UNROLL)
        place[:WINDOW] = total
        place[WINDOW:] = square

    def finish(f, b, tall, target, base):
        top = pl.multiple_of(b * WINDOW, WINDOW)
        base = pl.multiple_of(base, WINDOW)
        middle, factor = tall[:WINDOW], tall[WINDOW:]

        @pl.loop(0, chunks, unroll=UNROLL)
        def chunk(c):
            cols = columns(c)
            clipped = rolling[f, pl.ds(top, WINDOW), cols]
            deviate = (clipped - middle) * weight[pl.ds(top + WINDOW, WINDOW), cols]
            target[pl.ds(base, WINDOW), cols] = deviate * factor

    def places(g):
        start, size = groups[g]
        number = size * (blocks - 1)
        where = [(start + i % size, 1 + i // size) for i in range(number)]
        if start + size == fields:
            where.append((ahead, 0))
        return where

    def items(g):
        start, size = groups[g]
        whole = size * (blocks - 1)
        if start + size < fields:
            return whole, lambda i: (start + lax.rem(i, size), 1 + lax.div(i, size))
        return whole + is_first.astype(jnp.int32), lambda i: (
            jnp.where(i < whole, start + lax.rem(i, size), ahead),
            jnp.where(i < whole, 1 + lax.div(i, size), 0),
        )

    def gather_rows(g, slot):
        for i in range(len(places(g))):
            part[slot, pl.ds(i, 1), :] = row_of(lanes[1 + g, i])
        send(slot)

    def spread_rows(g, slot):
        total = receive(slot)
        number = len(places(g))
        count = jnp.concatenate([totals[pl.ds(b, 1), :] for _, b in places(g)], axis=0)
        rows_of = factor_rows(total[:number], count)
        for i in range(number):
            spread[g, i] = upright(rows_of[i : i + 1])

    def meet_plane():
        for i in range(blocks + 1):
            part[0, pl.ds(i, 1), :] = row_of(lanes[0, i])
        pl.semaphore_wait(ready, len(cross_peers))
        send(0)

    def main_first(g):
        start, size = groups[g]
        for f in range(start, start + size):
            loads[f].wait()
        number, place = items(g)

        @pl.loop(0, number)
        def item(i):
            f, b = place(i)
            roll_window(f, b, lanes.at[1 + g, i])

        if g == 0:
            meet_plane()
        gather_rows(g, 1 + 2 * g)

    def main_second(g):
        spread_rows(g, 1 + 2 * g)
        number, place = items(g)

        @pl.loop(0, number)
        def item(i):
            f, b = place(i)
            clip_scores(f, b, spread[g, i], lanes.at[1 + g, i])

        gather_rows(g, 2 + 2 * g)

    def main_third(g):
        spread_rows(g, 2 + 2 * g)
        number, place = items(g)

        @pl.loop(0, number)
        def item(i):
            f, b = place(i)
            finish(f, b, spread[g, i], out.at[f], b * WINDOW)

    single = lanes.at[0, 0]

    def tail_first(f, b):
        roll_window(f, b, single)
        tail_part[2 * f] = row_of(single[...])
        send_row(2 * f)

    def tail_factors(slot, b):
        return upright(factor_rows(receive_row(slot), totals[pl.ds(b, 1), :]))

    def tail_second(f, b):
        clip_scores(f, b, tail_factors(2 * f, b), single)
        tail_part[2 * f + 1] = row_of(single[...])
        send_row(2 * f + 1)

    def tail_third(f, b, target):
        finish(f, b, tail_factors(2 * f + 1, b), target, 0)

    def ahead_first():
        upcoming.wait_recv()
        tail_first(ahead, blocks)

    def ahead_second():
        tail_second(ahead, blocks)

    def ahead_third():
        tail_third(ahead, blocks, stage)
        finished.start()

    not_last = pl.when(jnp.logical_not(is_last))

    def relay(arriving, leaving, k):
        def pass_on():
            arriving[k].wait_recv()
            leaving[k].start()

        return pass_on

    def first(f):
        waits = [(halos[k].wait_recv, start, width) for k, (g, start, width) in enumerate(pieces) if g == f]
        if f == ahead - 1:
            waits += [
                (cross_onward[k].wait_recv, DIRECT + k * share, share) for k in range(RELAYS)
            ]
        begin = (zero, zero)
        for wait, start, width in waits:
            pl.when(jnp.logical_not(is_first))(wait)
            roll_window(f, 0, single, start // LANES, (start + width) // LANES, begin)
            begin = (single[:WINDOW], single[WINDOW:])
        tail_part[2 * f] = row_of(single[...])
        send_row(2 * f)

    def second(f):
        tail_second(f, 0)

    def third(f):
        tail_third(f, 0, out.at[f])

    main_first(0)
    main_first(1)
    totals[...] = receive(0)
    main_second(0)
    not_last(ahead_first)
    first(0)
    pl.when(is_last)(relay(even_detour, cross_onward, 0))
    main_second(1)
    pl.when(is_last)(relay(even_detour, cross_onward, 1))
    main_third(0)
    pl.when(is_last)(relay(even_detour, cross_onward, 2))
    not_last(ahead_second)
    pl.when(tm == 1)(relay(even_detour, cross_onward, 0))
    pl.when(is_last)(relay(odd_detour, back_onward, 0))
    pl.when(is_last)(relay(odd_detour, back_onward, 1))
    second(0)
    pl.when(tm == 1)(relay(even_detour, cross_onward, 1))
    pl.when(is_last)(relay(odd_detour, back_onward, 2))
    main_third(1)
    pl.when(tm == 1)(relay(even_detour, cross_onward, 2))
    not_last(ahead_third)
    first(1)
    first(2)
    third(0)
    second(1)
    second(2)
    third(1)
    third(2)

    @pl.when(jnp.logical_not(is_first))
    def arrivals():
        finished.wait_recv()
        upcoming.wait_send()

    for k in range(RELAYS):
        pl.when(jnp.logical_not(is_last))(even_detour[k].wait_send)
        pl.when(jnp.logical_not(is_even))(cross_onward[k].wait_send)
        pl.when(is_last)(back_onward[k].wait_send)
    for copy in halos:
        pl.when(jnp.logical_not(is_last))(copy.wait_send)
    for slot in range(part.shape[0]):
        sent = got.at[slot]
        pltpu.make_async_copy(sent, sent, send_sem.at[slot]).wait()

    def row_sent(slot):
        sent = tail_got.at[slot]
        pltpu.make_async_copy(sent, sent, tail_send.at[slot]).wait()

    for slot in range(2 * ahead):
        row_sent(slot)

    @not_last
    def departures():
        finished.wait_send()
        row_sent(2 * ahead)
        row_sent(2 * ahead + 1)


def per_device(n_tm, n_as, values, listed_from, listed_until):
    fields, rows, assets = values.shape
    blocks = rows // WINDOW
    groups = field_groups(fields)
    stats = -(-max(groups[0][1] * (blocks - 1) + 1, blocks + 2) // 8) * 8
    slots = 1 + 2 * len(groups)
    f32 = jnp.float32
    vmem = pltpu.VMEM
    dma = pltpu.SemaphoreType.DMA
    return pl.pallas_call(
        functools.partial(kernel, n_tm, n_as),
        out_shape=vmem((fields, rows, assets), f32),
        in_specs=[pl.BlockSpec(memory_space=pltpu.HBM)] * 3,
        out_specs=pl.BlockSpec(memory_space=vmem),
        scratch_shapes=[
            vmem((fields, rows + 2 * WINDOW, assets), f32),
            vmem((fields, rows + WINDOW, assets), f32),
            vmem((rows + 2 * WINDOW, assets), f32),
            vmem((rows + 2 * WINDOW, assets), f32),
            vmem((1, assets), jnp.int32),
            vmem((1, assets), jnp.int32),
            vmem((WINDOW, assets), f32),
            vmem((2, RELAYS, WINDOW, (assets - DIRECT) // RELAYS), f32),
            vmem((1 + len(groups), stats, LANES, LANES), f32),
            vmem((len(groups), stats, LANES, LANES), f32),
            vmem((slots, stats, LANES), f32),
            vmem((slots, n_as - 1, stats, LANES), f32),
            vmem((stats, LANES), f32),
            vmem((2 * fields, 1, LANES), f32),
            vmem((2 * fields, n_as - 1, LANES), f32),
            dma((fields + 2,)),
            dma((fields - 2 + PIECES,)),
            dma((fields - 2 + PIECES,)),
            dma((2,)),
            dma((2,)),
            dma((RELAYS,)),
            dma((2, RELAYS)),
            dma((2, RELAYS)),
            dma((RELAYS,)),
            pltpu.SemaphoreType.REGULAR,
            dma((slots,)),
            dma((slots,)),
            dma((2 * fields,)),
            dma((2 * fields,)),
        ],
        compiler_params=pltpu.CompilerParams(
            collective_id=0, has_side_effects=True, vmem_limit_bytes=48 * 2**20
        ),
    )(values, listed_from[None], listed_until[None])


def solution(mesh):
    in_specs = (P(None, "tm", "asset"), P("asset"), P("asset"))
    out_specs = P(None, "tm", "asset")
    body = functools.partial(per_device, mesh.shape["tm"], mesh.shape["asset"])
    return jax.shard_map(
        body, mesh=mesh, in_specs=in_specs, out_specs=out_specs, check_vma=False
    )
```
